32 devices in a mesh: dp: 2 (over z, core), sp: 16 (over x, y).
Axes of the slice: x: 4, y: 4, z: 1, core: 2. Of those that a mesh axis runs over, the one named last changes fastest.
The devices are a block of a 4x4x8 slice.
Arguments:
- q: bfloat16 [64, 16, 128], P('dp'), parts along dimension 0
- k: bfloat16 [64, 8192, 16, 128], P('dp', 'sp'), parts along dimension 0
- v: bfloat16 [64, 8192, 16, 128], P('dp', 'sp'), parts along dimension 0
Outputs:
- q: bfloat16 [64, 16, 128], P('dp'), parts along dimension 0
There are 2 independent parts. The reference program is written for one: setup_inputs(seed, part) draws one part's arguments, and reference() takes and returns one part's arrays. A program takes and returns all parts, laid end to end along the dimension named above; each array names one.
All inputs are finite; a program needn't handle non-finite values.
Results may differ from the reference program's by a relative error of at most 0.012.
Values are sent between devices in bfloat16 or wider.
A program may use at most 768 MiB of HBM per device.

```python
import jax
import jax.numpy as jnp

BATCH = 32
CACHE = 8192
HEADS = 16
KV_HEADS = 16
HEAD = 128


def setup_inputs(seed: int = 0, part: int = 0) -> dict:
    kq, kk, kv = (jax.random.fold_in(k, part) for k in jax.random.split(jax.random.key(seed), 3))
    return {
        "q": (3 * jax.random.normal(kq, (BATCH, HEADS, HEAD), jnp.float32)).astype(jnp.bfloat16),
        "k": jax.random.normal(kk, (BATCH, CACHE, KV_HEADS, HEAD), jnp.float32).astype(jnp.bfloat16),
        "v": jax.random.normal(kv, (BATCH, CACHE, KV_HEADS, HEAD), jnp.float32).astype(jnp.bfloat16),
    }


def einsum(form, a, b):
    return jnp.einsum(form, a.astype(jnp.float32), b.astype(jnp.float32))


def reference(q, k, v):
    grouped = q.reshape(BATCH, KV_HEADS, -1, HEAD)
    scores = einsum("bgsd,bugd->bgsu", grouped, k) * HEAD**-0.5
    weights = jax.nn.softmax(scores, -1).astype(jnp.bfloat16)
    return einsum("bgsu,bugd->bgsd", weights, v).astype(jnp.bfloat16).reshape(BATCH, HEADS, HEAD)
```

```python
import functools

import jax
import jax.numpy as jnp
from jax import lax
from jax.experimental import pallas as pl
from jax.experimental.pallas import tpu as pltpu
from jax.sharding import PartitionSpec as P

SLOTS = 3
GROUP = 2
LAG = 4
TILE = 256
LOG2E = 1.4426950408889634


def attend(q, k, v, scores, scale):
    heads, head = q.shape
    rows = k.shape[0]
    half = rows // 2
    zero = jnp.zeros_like(q)
    twice = jnp.concatenate([jnp.concatenate([q, zero], 1), jnp.concatenate([zero, q], 1)], 0)
    shape = (2 * heads, TILE)
    own = lax.broadcasted_iota(jnp.int32, shape, 0) % heads == lax.broadcasted_iota(jnp.int32, shape, 1) % heads
    high = jnp.full(shape, -jnp.inf, jnp.float32)
    for i in range(half // TILE):
        keys = jnp.concatenate([k[pl.ds(i * TILE, TILE), :], k[pl.ds(half + i * TILE, TILE), :]], 1)
        s = lax.dot_general(twice, keys, (((1,), (1,)), ((), ())), preferred_element_type=jnp.float32)
        s = jnp.where(own, s, -jnp.inf)
        scores[:, pl.ds(i * TILE, TILE)] = s
        high = jnp.maximum(high, s)
    top = jnp.max(high, 1, keepdims=True)
    top = jnp.maximum(top[:heads], top[heads:])
    both = jnp.concatenate([top, top], 0)
    total = jnp.zeros(shape, jnp.float32)
    seen = jnp.zeros((2 * heads, 2 * head), jnp.float32)
    for i in range(half // TILE):
        w = jnp.exp2((scores[:, pl.ds(i * TILE, TILE)] - both) * (scale * LOG2E))
        total = total + w
        values = jnp.concatenate([v[pl.ds(i * TILE, TILE), :], v[pl.ds(half + i * TILE, TILE), :]], 1)
        seen = seen + jnp.dot(w.astype(jnp.bfloat16), values, preferred_element_type=jnp.float32)
    total = jnp.sum(total, 1, keepdims=True)
    return seen[:heads, :head] + seen[heads:, head:], top, total[:heads] + total[heads:]


def kernel(
    n, scale, q_ref, k_ref, v_ref, out_ref, k_buf, v_buf, scores_a, scores_b, parts, stats, k_sem, v_sem, send_sem, recv_sem, stat_send_sem, stat_recv_sem
):
    me = lax.axis_index("sp")
    sequences, heads, head = q_ref.shape
    groups = sequences // GROUP
    lanes = lax.broadcasted_iota(jnp.int32, (8, 128), 1)

    def fetch(g, start):
        slot = lax.rem(g, SLOTS)
        for hbm, buf, sem in ((k_ref, k_buf, k_sem), (v_ref, v_buf, v_sem)):
            for j in range(GROUP):
                copy = pltpu.make_async_copy(hbm.at[g * GROUP + j], buf.at[slot, j], sem.at[slot, j])
                copy.start() if start else copy.wait()

    for g in range(SLOTS):
        fetch(g, True)

    barrier = pltpu.get_barrier_semaphore()
    for d in range(1, n):
        pl.semaphore_signal(barrier, inc=1, device_id={"sp": lax.rem(me + d, n)}, device_id_type=pl.DeviceIdType.MESH)

    def send(g):
        @pl.loop(1, n)
        def _(d):
            peer = {"sp": lax.rem(me + d, n)}
            for buf, s_sem, r_sem in ((parts, send_sem, recv_sem), (stats, stat_send_sem, stat_recv_sem)):
                pltpu.make_async_remote_copy(
                    src_ref=buf.at[g, me], dst_ref=buf.at[g, me], send_sem=s_sem.at[g], recv_sem=r_sem.at[g], device_id=peer, device_id_type=pl.DeviceIdType.MESH
                ).start()

    def wait_all(buf, sem, g):
        whole = buf.at[g, pl.ds(0, n - 1)]
        pltpu.make_async_copy(whole, whole, sem.at[g]).wait()

    def combine(g):
        wait_all(parts, recv_sem, g)
        wait_all(stats, stat_recv_sem, g)
        stat = [stats[g, p] for p in range(n)]
        high = functools.reduce(jnp.maximum, stat)
        weight = [jnp.exp2((s - high) * (scale * LOG2E)) for s in stat]
        sums = [pltpu.roll(s, 126, 1) for s in stat]
        total = functools.reduce(jnp.add, [a * b for a, b in zip(weight, sums)])
        share = [w / total for w in weight]
        for j in range(GROUP):
            acc = [jnp.zeros((8, head), jnp.float32)] * 2
            for p in range(n):
                part = parts[g, p, j].astype(jnp.float32)
                for h in range(2):
                    lane = 4 * j + h
                    acc[h] = acc[h] + part[8 * h : 8 * h + 8] * share[p][:, lane : lane + 1]
            out_ref[g * GROUP + j] = jnp.concatenate(acc, 0).astype(out_ref.dtype)

    @pl.loop(0, groups)
    def _(g):
        slot = lax.rem(g, SLOTS)
        fetch(g, False)
        stat = jnp.zeros((8, 128), jnp.float32)
        for j, scores in enumerate((scores_a, scores_b)):
            seen, top, total = attend(q_ref[g * GROUP + j], k_buf.at[slot, j], v_buf.at[slot, j], scores, scale)
            parts[g, me, j] = seen.astype(parts.dtype)
            for lane, value in enumerate((top[:8], top[8:], total[:8], total[8:])):
                stat = jnp.where(lanes == 4 * j + lane, value, stat)
        stats[g, me] = stat

        @pl.when(g + SLOTS < groups)
        def _():
            fetch(g + SLOTS, True)

        @pl.when(g == 0)
        def _():
            pl.semaphore_wait(barrier, n - 1)

        send(g)

        @pl.when(g >= LAG)
        def _():
            combine(g - LAG)

    @pl.loop(groups - LAG, groups)
    def _(g):
        combine(g)

    @pl.loop(0, groups)
    def _(g):
        wait_all(parts, send_sem, g)
        wait_all(stats, stat_send_sem, g)


def solution(mesh):
    n = mesh.shape["sp"]

    def step(q, k, v):
        b, t, h, d = k.shape
        groups = b // GROUP
        return pl.pallas_call(
            functools.partial(kernel, n, d**-0.5),
            out_shape=jax.ShapeDtypeStruct(q.shape, q.dtype),
            in_specs=[pl.BlockSpec(memory_space=pltpu.VMEM), pl.BlockSpec(memory_space=pl.ANY), pl.BlockSpec(memory_space=pl.ANY)],
            out_specs=pl.BlockSpec(memory_space=pltpu.VMEM),
            scratch_shapes=[
                pltpu.VMEM((SLOTS, GROUP, t * h, d), k.dtype),
                pltpu.VMEM((SLOTS, GROUP, t * h, d), v.dtype),
                pltpu.VMEM((2 * h, t * h // 2), jnp.float32),
                pltpu.VMEM((2 * h, t * h // 2), jnp.float32),
                pltpu.VMEM((groups, n, GROUP, h, d), jnp.bfloat16),
                pltpu.VMEM((groups, n, 8, 128), jnp.float32),
                pltpu.SemaphoreType.DMA((SLOTS, GROUP)),
                pltpu.SemaphoreType.DMA((SLOTS, GROUP)),
                pltpu.SemaphoreType.DMA((groups,)),
                pltpu.SemaphoreType.DMA((groups,)),
                pltpu.SemaphoreType.DMA((groups,)),
                pltpu.SemaphoreType.DMA((groups,)),
            ],
            compiler_params=pltpu.CompilerParams(collective_id=0, has_side_effects=True, vmem_limit_bytes=60 * 2**20),
        )(q, k.reshape(b, t * h, d), v.reshape(b, t * h, d))

    return jax.shard_map(
        step,
        mesh=mesh,
        in_specs=(P("dp", None, None), P("dp", "sp", None, None), P("dp", "sp", None, None)),
        out_specs=P("dp", None, None),
        check_vma=False,
    )
```

```python
import functools

import jax
import jax.numpy as jnp
from jax import lax
from jax.experimental import pallas as pl
from jax.experimental.pallas import tpu as pltpu
from jax.sharding import PartitionSpec as P

SLOTS = 6
CHUNK = 4
LAST = (2, 1, 1)
BLOCK = 2
TILE = 256
LOG2E = 1.4426950408889634
SIDE = 4


def side_by_side(ref, i):
    half = ref.shape[0] // 2
    return jnp.concatenate([ref[pl.ds(i * TILE, TILE), :], ref[pl.ds(half + i * TILE, TILE), :]], 1)


def score(q, k, scores, result):
    heads = q.shape[0]
    zero = jnp.zeros_like(q)
    twice = jnp.concatenate([jnp.concatenate([q, zero], 1), jnp.concatenate([zero, q], 1)], 0)
    shape = (2 * heads, TILE)
    own = lax.broadcasted_iota(jnp.int32, shape, 0) % heads == lax.broadcasted_iota(jnp.int32, shape, 1) % heads
    high = jnp.full(shape, -jnp.inf, jnp.float32)
    for i in range(scores.shape[1] // TILE):
        s = lax.dot_general(twice, side_by_side(k, i), (((1,), (1,)), ((), ())), preferred_element_type=jnp.float32)
        s = jnp.where(own, s, -jnp.inf)
        scores[:, pl.ds(i * TILE, TILE)] = s
        high = jnp.maximum(high, s)
        yield
    top = jnp.max(high, 1, keepdims=True)
    top = jnp.maximum(top[:heads], top[heads:])
    result.append(jnp.concatenate([top, top], 0))


def weigh(scores, top, v, scale, result):
    heads, head = scores.shape[0] // 2, v.shape[1]
    total = jnp.zeros((2 * heads, TILE), jnp.float32)
    seen = jnp.zeros((2 * heads, 2 * head), jnp.float32)
    for i in range(scores.shape[1] // TILE):
        w = jnp.exp2((scores[:, pl.ds(i * TILE, TILE)] - top) * (scale * LOG2E))
        total = total + w
        seen = seen + jnp.dot(w.astype(jnp.bfloat16), side_by_side(v, i), preferred_element_type=jnp.float32)
        yield
    total = jnp.sum(total, 1, keepdims=True)
    result.extend((seen[:heads, :head] + seen[heads:, head:], total[:heads] + total[heads:]))


def together(*steps):
    live = list(steps)
    while live:
        live = [s for s in live if next(s, live) is not live]


def kernel(scale, q_ref, k_ref, v_ref, out_ref, k_buf, v_buf, scores_a, scores_b, tops, parts, stats, k_sem, v_sem, send_sem, recv_sem, stat_send_sem, stat_recv_sem):
    me = lax.axis_index("sp")
    place = (lax.div(me, SIDE), lax.rem(me, SIDE))
    sequences, heads, head = q_ref.shape
    chunks = sequences // CHUNK
    scores = (scores_a, scores_b)
    lanes = lax.broadcasted_iota(jnp.int32, (8, 128), 1)

    def key_copy(s):
        slot = lax.rem(s, SLOTS)
        return pltpu.make_async_copy(k_ref.at[s], k_buf.at[slot], k_sem.at[slot])

    def value_copy(s):
        slot = lax.rem(s, SLOTS)
        return pltpu.make_async_copy(v_ref.at[s], v_buf.at[slot], v_sem.at[slot])

    def peer(axis, d):
        x, y = place
        return {"sp": lax.rem(x + d, SIDE) * SIDE + y if axis == 0 else x * SIDE + lax.rem(y + d, SIDE)}

    for s in range(SLOTS):
        key_copy(s).start()
        value_copy(s).start()

    barrier = pltpu.get_barrier_semaphore()
    for axis in range(2):
        for d in range(1, SIDE):
            pl.semaphore_signal(barrier, inc=1, device_id=peer(axis, d), device_id_type=pl.DeviceIdType.MESH)

    def send(axis, c, s, count):
        mine = place[axis]
        for d in range(1, SIDE):
            for ref, s_sem, r_sem in (
                (parts.at[axis, mine, pl.ds(s, count)], send_sem, recv_sem),
                (stats.at[axis, c, mine], stat_send_sem, stat_recv_sem),
            ):
                pltpu.make_async_remote_copy(
                    src_ref=ref, dst_ref=ref, send_sem=s_sem.at[axis, c], recv_sem=r_sem.at[axis, c], device_id=peer(axis, d), device_id_type=pl.DeviceIdType.MESH
                ).start()

    def wait_all(axis, c, s, count, sem, stat_sem):
        for ref, sem in ((parts.at[axis, pl.ds(0, SIDE - 1), pl.ds(s, count)], sem), (stats.at[axis, c, pl.ds(0, SIDE - 1)], stat_sem)):
            pltpu.make_async_copy(ref, ref, sem.at[axis, c]).wait()

    def put(axis, c, s, count, sums, stat):
        for j in range(count):
            parts[axis, place[axis], s + j] = sums[j].astype(parts.dtype)
        stats[axis, c, place[axis]] = stat

    def combine(axis, c, s, count):
        wait_all(axis, c, s, count, recv_sem, stat_recv_sem)
        stat = [stats[axis, c, p] for p in range(SIDE)]
        high = functools.reduce(jnp.maximum, stat)
        weight = [jnp.exp2((t - high) * (scale * LOG2E)) for t in stat]
        total = functools.reduce(jnp.add, [a * pltpu.roll(t, 126, 1) for a, t in zip(weight, stat)])
        if axis == 1:
            weight = [w / total for w in weight]
        sums = []
        for j in range(count):
            acc = [jnp.zeros((8, head), jnp.float32)] * 2
            for p in range(SIDE):
                part = parts[axis, p, s + j].astype(jnp.float32)
                for h in range(2):
                    lane = 4 * j + h
                    acc[h] = acc[h] + part[8 * h : 8 * h + 8] * weight[p][:, lane : lane + 1]
            sums.append(jnp.concatenate(acc, 0))
        if axis == 0:
            put(1, c, s, count, sums, jnp.where(lanes % 4 < 2, high, pltpu.roll(total, 2, 1)))
        else:
            for j in range(count):
                out_ref[s + j] = sums[j].astype(out_ref.dtype)

    def attend(first, keys, values, sums, stat, base):
        for j in keys:
            key_copy(first + j).wait()
        for j in values:
            value_copy(first + j).wait()
        for j in sorted({*(j - 1 for j in keys), *values}):
            top, result, steps = [], [], []
            if j + 1 in keys:
                steps.append(score(q_ref[first + j + 1], k_buf.at[lax.rem(first + j + 1, SLOTS)], scores[(j + 1) % 2], top))
            if j in values:
                high = tops[j % 2]
                steps.append(weigh(scores[j % 2], high, v_buf.at[lax.rem(first + j, SLOTS)], scale, result))
            together(*steps)
            if top:
                tops[(j + 1) % 2] = top[0]
            if result:
                sums.append(result[0])
                for lane, value in enumerate((high[:8], high[8:16], result[1][:8], result[1][8:])):
                    stat = jnp.where(lanes == 4 * (j - base) + lane, value, stat)
        return stat

    def refill(copy, s):
        @pl.when(s < sequences)
        def _():
            copy(s).start()

    def none():
        return jnp.zeros((8, 128), jnp.float32)

    attend(0, [0], [], [], none(), 0)
    key_copy(SLOTS).start()

    @pl.loop(0, chunks - 1)
    def _(c):
        first = c * CHUNK
        sums, stat = [], none()
        for j in range(0, CHUNK, BLOCK):
            stat = attend(first, list(range(j + 1, j + BLOCK + 1)), list(range(j, j + BLOCK)), sums, stat, 0)
            for i in range(j, j + BLOCK):
                refill(key_copy, first + i + 1 + SLOTS)
                refill(value_copy, first + i + SLOTS)
        put(0, c, first, CHUNK, sums, stat)

        @pl.when(c == 0)
        def _():
            pl.semaphore_wait(barrier, 2 * (SIDE - 1))

        send(0, c, first, CHUNK)

        @pl.when(c >= 1)
        def _():
            combine(0, c - 1, first - CHUNK, CHUNK)
            send(1, c - 1, first - CHUNK, CHUNK)

        @pl.when(c >= 2)
        def _():
            combine(1, c - 2, first - 2 * CHUNK, CHUNK)

    first = sequences - CHUNK
    pieces = []
    done = 0
    for i, count in enumerate(LAST):
        sums, stat = [], none()
        for j in range(done, done + count):
            stat = attend(first, [j + 1] if j + 1 < CHUNK else [], [j], sums, stat, done)
        piece = (chunks - 1 + i, first + done, count)
        put(0, *piece, sums, stat)
        send(0, *piece)
        pieces.append(piece)
        done += count
        if i == 0:
            combine(0, chunks - 2, first - CHUNK, CHUNK)
            send(1, chunks - 2, first - CHUNK, CHUNK)
            combine(1, chunks - 3, first - 2 * CHUNK, CHUNK)
    for piece in pieces:
        combine(0, *piece)
        send(1, *piece)
    combine(1, chunks - 2, first - CHUNK, CHUNK)
    for piece in pieces:
        combine(1, *piece)

    for axis in range(2):

        @pl.loop(0, chunks - 1)
        def _(c):
            wait_all(axis, c, c * CHUNK, CHUNK, send_sem, stat_send_sem)

        for piece in pieces:
            wait_all(axis, *piece, send_sem, stat_send_sem)


def solution(mesh):
    def step(q, k, v):
        b, t, h, d = k.shape
        pieces = b // CHUNK - 1 + len(LAST)
        dma = pltpu.SemaphoreType.DMA
        return pl.pallas_call(
            functools.partial(kernel, d**-0.5),
            out_shape=jax.ShapeDtypeStruct(q.shape, q.dtype),
            in_specs=[pl.BlockSpec(memory_space=pltpu.VMEM), pl.BlockSpec(memory_space=pl.ANY), pl.BlockSpec(memory_space=pl.ANY)],
            out_specs=pl.BlockSpec(memory_space=pltpu.VMEM),
            scratch_shapes=[
                pltpu.VMEM((SLOTS, t * h, d), k.dtype),
                pltpu.VMEM((SLOTS, t * h, d), v.dtype),
                pltpu.VMEM((2 * h, t * h // 2), jnp.float32),
                pltpu.VMEM((2 * h, t * h // 2), jnp.float32),
                pltpu.VMEM((2, 2 * h, 1), jnp.float32),
                pltpu.VMEM((2, SIDE, b, h, d), jnp.bfloat16),
                pltpu.VMEM((2, pieces, SIDE, 8, 128), jnp.float32),
                dma((SLOTS,)),
                dma((SLOTS,)),
                dma((2, pieces)),
                dma((2, pieces)),
                dma((2, pieces)),
                dma((2, pieces)),
            ],
            compiler_params=pltpu.CompilerParams(collective_id=0, has_side_effects=True, vmem_limit_bytes=60 * 2**20),
        )(q, k.reshape(b, t * h, d), v.reshape(b, t * h, d))

    return jax.shard_map(
        step,
        mesh=mesh,
        in_specs=(P("dp", None, None), P("dp", "sp", None, None), P("dp", "sp", None, None)),
        out_specs=P("dp", None, None),
        check_vma=False,
    )
```

```python
import functools
import math

import jax
import jax.numpy as jnp
from jax import lax
from jax.experimental import pallas as pl
from jax.experimental.pallas import tpu as pltpu
from jax.sharding import PartitionSpec as P

SLOTS = 6
CHUNK = 4
LEAD = 2
EARLY = 3
LAG = 3
TILE = 256
LOG2E = 1.4426950408889634


def side_by_side(ref, i):
    half = ref.shape[0] // 2
    return jnp.concatenate([ref[pl.ds(i * TILE, TILE), :], ref[pl.ds(half + i * TILE, TILE), :]], 1)


def score(q, k, scores, result):
    heads = q.shape[0]
    zero = jnp.zeros_like(q)
    twice = jnp.concatenate([jnp.concatenate([q, zero], 1), jnp.concatenate([zero, q], 1)], 0)
    shape = (2 * heads, TILE)
    own = lax.broadcasted_iota(jnp.int32, shape, 0) % heads == lax.broadcasted_iota(jnp.int32, shape, 1) % heads
    high = jnp.full(shape, -jnp.inf, jnp.float32)
    for i in range(scores.shape[1] // TILE):
        s = lax.dot_general(twice, side_by_side(k, i), (((1,), (1,)), ((), ())), preferred_element_type=jnp.float32)
        s = jnp.where(own, s, -jnp.inf)
        scores[:, pl.ds(i * TILE, TILE)] = s
        high = jnp.maximum(high, s)
        yield
    result.append(high)


def weigh(scores, high, v, scale, result):
    heads, head = scores.shape[0] // 2, v.shape[1]
    top = jnp.max(high, 1, keepdims=True)
    top = jnp.maximum(top[:heads], top[heads:])
    both = jnp.concatenate([top, top], 0)
    total = jnp.zeros((2 * heads, TILE), jnp.float32)
    seen = [jnp.zeros((2 * heads, 2 * head), jnp.float32)] * 2
    for i in range(scores.shape[1] // TILE):
        w = jnp.exp2((scores[:, pl.ds(i * TILE, TILE)] - both) * (scale * LOG2E))
        total = total + w
        seen[i % 2] = seen[i % 2] + jnp.dot(w.astype(jnp.bfloat16), side_by_side(v, i), preferred_element_type=jnp.float32)
        yield
    total, seen = jnp.sum(total, 1, keepdims=True), seen[0] + seen[1]
    result.extend((seen[:heads, :head] + seen[heads:, head:], top, total[:heads] + total[heads:]))


def in_turn(steps):
    for step in steps:
        yield from step


def together(*steps):
    live = list(steps)
    while live:
        live = [s for s in live if next(s, live) is not live]


def kernel(
    side, scale, q_hbm, k_ref, v_ref, out_ref, q_ref, k_buf, v_buf, scores, tops, parts, stats, end_parts, end_stats, q_sem, k_sem, v_sem, send_sem, recv_sem, stat_send_sem, stat_recv_sem, end_sem
):
    me = lax.axis_index("sp")
    place = (lax.div(me, side), lax.rem(me, side))
    sequences, heads, head = q_ref.shape
    chunks = sequences // CHUNK
    ring = sorted(range(1, side), key=lambda d: -min(d, side - d))
    others = sorted(((dx, dy) for dx in range(side) for dy in range(side) if dx or dy), key=lambda d: -sum(min(i, side - i) for i in d))
    lanes = lax.broadcasted_iota(jnp.int32, (8, 128), 1)

    def key_copy(s):
        slot = lax.rem(s, SLOTS)
        return pltpu.make_async_copy(k_ref.at[s], k_buf.at[slot], k_sem.at[slot])

    def value_copy(s):
        slot = lax.rem(s, SLOTS)
        return pltpu.make_async_copy(v_ref.at[s], v_buf.at[slot], v_sem.at[slot])

    def peer(dx, dy):
        x, y = place
        return {"sp": lax.rem(x + dx, side) * side + lax.rem(y + dy, side)}

    q_copy = pltpu.make_async_copy(q_hbm, q_ref, q_sem)
    q_copy.start()
    for s in range(EARLY):
        key_copy(s).start()

    barrier = pltpu.get_barrier_semaphore()
    for d in others:
        pl.semaphore_signal(barrier, inc=1, device_id=peer(*d), device_id_type=pl.DeviceIdType.MESH)

    def send(axis, c, s, count):
        mine = place[axis]
        for d in ring:
            for ref, s_sem, r_sem in (
                (parts.at[axis, mine, pl.ds(s, count)], send_sem, recv_sem),
                (stats.at[axis, c, mine], stat_send_sem, stat_recv_sem),
            ):
                pltpu.make_async_remote_copy(
                    src_ref=ref, dst_ref=ref, send_sem=s_sem, recv_sem=r_sem.at[axis, c], device_id=peer(d, 0) if axis == 0 else peer(0, d), device_id_type=pl.DeviceIdType.MESH
                ).start()

    def arrive(axis, c, s, count):
        for ref, sem in ((parts.at[axis, pl.ds(0, side - 1), pl.ds(s, count)], recv_sem), (stats.at[axis, c, pl.ds(0, side - 1)], stat_recv_sem)):
            pltpu.make_async_copy(ref, ref, sem.at[axis, c]).wait()

    def put(axis, c, s, count, sums, stat):
        for j in range(count):
            parts[axis, place[axis], s + j] = sums[j].astype(parts.dtype)
        stats[axis, c, place[axis]] = stat

    def sums_of(stat, part, count, final):
        high = functools.reduce(jnp.maximum, stat)
        weight = [jnp.exp2((t - high) * (scale * LOG2E)) for t in stat]
        total = functools.reduce(jnp.add, [a * pltpu.roll(t, 126, 1) for a, t in zip(weight, stat)])
        if final:
            weight = [w / total for w in weight]
        sums = []
        for j in range(count):
            acc = [jnp.zeros((8, head), jnp.float32)] * 2
            for p, w in enumerate(weight):
                one = part(p, j).astype(jnp.float32)
                for h in range(2):
                    lane = 4 * j + h
                    acc[h] = acc[h] + one[8 * h : 8 * h + 8] * w[:, lane : lane + 1]
            sums.append(jnp.concatenate(acc, 0))
        return sums, jnp.where(lanes % 4 < 2, high, pltpu.roll(total, 2, 1))

    def combine(axis, c, s, count):
        arrive(axis, c, s, count)
        sums, stat = sums_of([stats[axis, c, p] for p in range(side)], lambda p, j: parts[axis, p, s + j], count, axis == 1)
        if axis == 0:
            put(1, c, s, count, sums, stat)
        else:
            for j in range(count):
                out_ref[s + j] = sums[j].astype(out_ref.dtype)

    def broadcast(ref, s_sem, r_sem):
        for d in others:
            pltpu.make_async_remote_copy(
                src_ref=ref, dst_ref=ref, send_sem=s_sem, recv_sem=r_sem, device_id=peer(*d), device_id_type=pl.DeviceIdType.MESH
            ).start()

    def attend(first, keys, values):
        for j in keys:
            key_copy(first + j).wait()
        for j in values:
            value_copy(first + j).wait()
        found, highs = [[] for _ in keys], [tops[j % len(scores)] for j in values]
        results = [[] for _ in values]
        together(
            in_turn([score(q_ref[first + j], k_buf.at[lax.rem(first + j, SLOTS)], scores[j % len(scores)], r) for j, r in zip(keys, found)]),
            in_turn([weigh(scores[j % len(scores)], high, v_buf.at[lax.rem(first + j, SLOTS)], scale, r) for j, high, r in zip(values, highs, results)]),
        )
        for j, (top,) in zip(keys, found):
            tops[j % len(scores)] = top
        return results

    def stat_of(rows):
        stat = jnp.zeros((8, 128), jnp.float32)
        for j, (_, high, total) in enumerate(rows):
            for lane, value in enumerate((high[:8], high[8:], total[:8], total[8:])):
                stat = jnp.where(lanes == 4 * j + lane, value, stat)
        return stat

    def refill(copy, s):
        @pl.when(s < sequences)
        def _():
            copy(s).start()

    q_copy.wait()
    for s in range(EARLY, SLOTS):
        value_copy(s - EARLY).start()
        key_copy(s).start()
    for s in range(SLOTS - EARLY, SLOTS):
        value_copy(s).start()
    for j in range(LEAD):
        attend(0, [j], [])
        key_copy(SLOTS + j).start()

    @pl.loop(0, chunks - 1)
    def _(c):
        first = c * CHUNK
        rows = []
        for j in range(CHUNK):
            rows += attend(first, [j + LEAD], [j])
            refill(key_copy, first + j + LEAD + SLOTS)
            refill(value_copy, first + j + SLOTS)
        put(0, c, first, CHUNK, [row[0] for row in rows], stat_of(rows))

        @pl.when(c == 0)
        def _():
            pl.semaphore_wait(barrier, len(others))

        send(0, c, first, CHUNK)

        @pl.when(c >= 1)
        def _():
            combine(0, c - 1, first - CHUNK, CHUNK)
            send(1, c - 1, first - CHUNK, CHUNK)

        @pl.when(c >= LAG)
        def _():
            combine(1, c - LAG, first - LAG * CHUNK, CHUNK)

    first = sequences - CHUNK
    last = (chunks - 2, first - CHUNK, CHUNK)
    rows = []
    for j in range(CHUNK):
        rows += attend(first, [j + LEAD] if j + LEAD < CHUNK else [], [j])
        end_parts[me, j] = rows[j][0].astype(end_parts.dtype)
        if j == CHUNK - 1:
            end_stats[me] = stat_of(rows)
            broadcast(end_stats.at[me], end_sem.at[1, 0], end_sem.at[1, 1])
        broadcast(end_parts.at[me, j], end_sem.at[0, 0], end_sem.at[0, 1])
    combine(0, *last)
    send(1, *last)
    for c in range(chunks - 1 - LAG, chunks - 1):
        combine(1, c, c * CHUNK, CHUNK)
    for i, ref in enumerate((end_parts, end_stats)):
        whole = ref.at[pl.ds(0, len(others))]
        pltpu.make_async_copy(whole, whole, end_sem.at[i, 1]).wait()
    sums, _ = sums_of([end_stats[p] for p in range(side * side)], lambda p, j: end_parts[p, j], CHUNK, True)
    for j in range(CHUNK):
        out_ref[first + j] = sums[j].astype(out_ref.dtype)

    for i, ref in enumerate((end_parts, end_stats)):
        whole = ref.at[pl.ds(0, len(others))]
        pltpu.make_async_copy(whole, whole, end_sem.at[i, 0]).wait()
    for ref, sem in ((parts.at[:, pl.ds(0, side - 1)], send_sem), (stats.at[:, :, pl.ds(0, side - 1)], stat_send_sem)):
        pltpu.make_async_copy(ref, ref, sem).wait()


def solution(mesh):
    side = math.isqrt(mesh.shape["sp"])

    def step(q, k, v):
        b, t, h, d = k.shape
        pieces = b // CHUNK - 1
        dma = pltpu.SemaphoreType.DMA
        return pl.pallas_call(
            functools.partial(kernel, side, d**-0.5),
            out_shape=pltpu.VMEM(q.shape, q.dtype),
            in_specs=[pl.BlockSpec(memory_space=pl.ANY)] * 3,
            out_specs=pl.BlockSpec(memory_space=pltpu.VMEM),
            scratch_shapes=[
                pltpu.VMEM((b, h, d), q.dtype),
                pltpu.VMEM((SLOTS, t * h, d), k.dtype),
                pltpu.VMEM((SLOTS, t * h, d), v.dtype),
                [pltpu.VMEM((2 * h, t * h // 2), jnp.float32)] * (2 * LEAD),
                pltpu.VMEM((2 * LEAD, 2 * h, TILE), jnp.float32),
                pltpu.VMEM((2, side, b - CHUNK, h, d), jnp.bfloat16),
                pltpu.VMEM((2, pieces, side, 8, 128), jnp.float32),
                pltpu.VMEM((side * side, CHUNK, h, d), jnp.bfloat16),
                pltpu.VMEM((side * side, 8, 128), jnp.float32),
                dma,
                dma((SLOTS,)),
                dma((SLOTS,)),
                dma,
                dma((2, pieces)),
                dma,
                dma((2, pieces)),
                dma((2, 2)),
            ],
            compiler_params=pltpu.CompilerParams(collective_id=0, has_side_effects=True, vmem_limit_bytes=60 * 2**20),
        )(q, k.reshape(b, t * h, d), v.reshape(b, t * h, d))

    return jax.shard_map(
        step,
        mesh=mesh,
        in_specs=(P("dp", None, None), P("dp", "sp", None, None), P("dp", "sp", None, None)),
        out_specs=P("dp", None, None),
        check_vma=False,
    )
```

```python
import functools
import math

import jax
import jax.numpy as jnp
from jax import lax
from jax.experimental import pallas as pl
from jax.experimental.pallas import tpu as pltpu
from jax.sharding import PartitionSpec as P

SLOTS = 6
CHUNK = 4
LEAD = 2
BLOCK = 1
EARLY = 3
LAG = 3
TILE = 256
END = ((0, 2), (2, 3), (3, 4))
TAIL = END[-1][1]
AFTER = 4
LOG2E = 1.4426950408889634


def side_by_side(ref, i):
    half = ref.shape[0] // 2
    return jnp.concatenate([ref[pl.ds(i * TILE, TILE), :], ref[pl.ds(half + i * TILE, TILE), :]], 1)


def score(q, k, scores, result):
    heads = q.shape[0]
    zero = jnp.zeros_like(q)
    twice = jnp.concatenate([jnp.concatenate([q, zero], 1), jnp.concatenate([zero, q], 1)], 0)
    shape = (2 * heads, TILE)
    own = lax.broadcasted_iota(jnp.int32, shape, 0) % heads == lax.broadcasted_iota(jnp.int32, shape, 1) % heads
    high = jnp.full(shape, -jnp.inf, jnp.float32)
    for i in range(scores.shape[1] // TILE):
        s = lax.dot_general(twice, side_by_side(k, i), (((1,), (1,)), ((), ())), preferred_element_type=jnp.float32)
        s = jnp.where(own, s, -jnp.inf)
        scores[:, pl.ds(i * TILE, TILE)] = s
        high = jnp.maximum(high, s)
        yield
    result.append(high)


def weigh(scores, high, v, scale, result):
    heads, head = scores.shape[0] // 2, v.shape[1]
    top = jnp.max(high, 1, keepdims=True)
    top = jnp.maximum(top[:heads], top[heads:])
    both = jnp.concatenate([top, top], 0)
    total = jnp.zeros((2 * heads, TILE), jnp.float32)
    seen = [jnp.zeros((2 * heads, 2 * head), jnp.float32)] * 2
    for i in range(scores.shape[1] // TILE):
        w = jnp.exp2((scores[:, pl.ds(i * TILE, TILE)] - both) * (scale * LOG2E))
        total = total + w
        seen[i % 2] = seen[i % 2] + jnp.dot(w.astype(jnp.bfloat16), side_by_side(v, i), preferred_element_type=jnp.float32)
        yield
    total, seen = jnp.sum(total, 1, keepdims=True), seen[0] + seen[1]
    result.extend((seen[:heads, :head] + seen[heads:, head:], top, total[:heads] + total[heads:]))


def sum_up(scores, high, scale, result):
    heads = scores.shape[0] // 2
    top = jnp.max(high, 1, keepdims=True)
    top = jnp.maximum(top[:heads], top[heads:])
    both = jnp.concatenate([top, top], 0)
    total = jnp.zeros((2 * heads, TILE), jnp.float32)
    for i in range(scores.shape[1] // TILE):
        total = total + jnp.exp2((scores[:, pl.ds(i * TILE, TILE)] - both) * (scale * LOG2E))
        yield
    total = jnp.sum(total, 1, keepdims=True)
    result.extend((top, total[:heads] + total[heads:]))


def in_turn(steps):
    for step in steps:
        yield from step


def together(*steps):
    live = list(steps)
    while live:
        live = [s for s in live if next(s, live) is not live]


def kernel(
    side, scale, q_hbm, k_ref, v_ref, out_ref, q_ref, k_buf, v_buf, scores, tops, parts, stats, end_parts, end_stats, q_sem, k_sem, v_sem, send_sem, recv_sem, stat_send_sem, stat_recv_sem, end_sem
):
    me = lax.axis_index("sp")
    place = (lax.div(me, side), lax.rem(me, side))
    sequences, heads, head = q_ref.shape
    chunks = (sequences - TAIL) // CHUNK
    ring = sorted(range(1, side), key=lambda d: -min(d, side - d))
    others = sorted(((dx, dy) for dx in range(side) for dy in range(side) if dx or dy), key=lambda d: -sum(min(i, side - i) for i in d))
    lanes = lax.broadcasted_iota(jnp.int32, (8, 128), 1)

    def key_copy(s):
        slot = lax.rem(s, SLOTS)
        return pltpu.make_async_copy(k_ref.at[s], k_buf.at[slot], k_sem.at[slot])

    def value_copy(s):
        slot = lax.rem(s, SLOTS)
        return pltpu.make_async_copy(v_ref.at[s], v_buf.at[slot], v_sem.at[slot])

    def peer(dx, dy):
        x, y = place
        return {"sp": lax.rem(x + dx, side) * side + lax.rem(y + dy, side)}

    q_copy = pltpu.make_async_copy(q_hbm, q_ref, q_sem)
    q_copy.start()
    for s in range(EARLY):
        key_copy(s).start()

    barrier = pltpu.get_barrier_semaphore()
    for d in others:
        pl.semaphore_signal(barrier, inc=1, device_id=peer(*d), device_id_type=pl.DeviceIdType.MESH)

    def send(axis, c, s, count):
        mine = place[axis]
        for d in ring:
            for ref, s_sem, r_sem in (
                (parts.at[axis, mine, pl.ds(s, count)], send_sem, recv_sem),
                (stats.at[axis, c, mine], stat_send_sem, stat_recv_sem),
            ):
                pltpu.make_async_remote_copy(
                    src_ref=ref, dst_ref=ref, send_sem=s_sem, recv_sem=r_sem.at[axis, c], device_id=peer(d, 0) if axis == 0 else peer(0, d), device_id_type=pl.DeviceIdType.MESH
                ).start()

    def arrive(axis, c, s, count):
        for ref, sem in ((parts.at[axis, pl.ds(0, side - 1), pl.ds(s, count)], recv_sem), (stats.at[axis, c, pl.ds(0, side - 1)], stat_recv_sem)):
            pltpu.make_async_copy(ref, ref, sem.at[axis, c]).wait()

    def put(axis, c, s, count, sums, stat):
        for j in range(count):
            parts[axis, place[axis], s + j] = sums[j].astype(parts.dtype)
        stats[axis, c, place[axis]] = stat

    def weights_of(stat, final):
        high = functools.reduce(jnp.maximum, stat)
        weight = [jnp.exp2((t - high) * (scale * LOG2E)) for t in stat]
        total = functools.reduce(jnp.add, [a * pltpu.roll(t, 126, 1) for a, t in zip(weight, stat)])
        if final:
            weight = [w / total for w in weight]
        return weight, jnp.where(lanes % 4 < 2, high, pltpu.roll(total, 2, 1))

    def sum_of(weight, part, j):
        acc = [jnp.zeros((8, head), jnp.float32)] * 2
        for p, w in enumerate(weight):
            one = part(p).astype(jnp.float32)
            for h in range(2):
                lane = 4 * j + h
                acc[h] = acc[h] + one[8 * h : 8 * h + 8] * w[:, lane : lane + 1]
        return jnp.concatenate(acc, 0)

    def combine(axis, c, s, count):
        arrive(axis, c, s, count)
        weight, stat = weights_of([stats[axis, c, p] for p in range(side)], axis == 1)
        sums = [sum_of(weight, lambda p: parts[axis, p, s + j], j) for j in range(count)]
        if axis == 0:
            put(1, c, s, count, sums, stat)
        else:
            for j in range(count):
                out_ref[s + j] = sums[j].astype(out_ref.dtype)

    def broadcast(ref, s_sem, r_sem):
        for d in others:
            pltpu.make_async_remote_copy(
                src_ref=ref, dst_ref=ref, send_sem=s_sem, recv_sem=r_sem, device_id=peer(*d), device_id_type=pl.DeviceIdType.MESH
            ).start()

    def attend(first, keys, values, ahead=None):
        for j in keys:
            key_copy(first + j).wait()
        for j in values:
            value_copy(first + j).wait()
        found, highs = [[] for _ in keys], [tops[j % len(scores)] for j in values]
        results = [[] for _ in values]
        if ahead is not None:
            results.append([None])
        scoring, weighing = (
            in_turn([score(q_ref[first + j], k_buf.at[lax.rem(first + j, SLOTS)], scores[j % len(scores)], r) for j, r in zip(keys, found)]),
            in_turn([weigh(scores[j % len(scores)], high, v_buf.at[lax.rem(first + j, SLOTS)], scale, r) for j, high, r in zip(values, highs, results)]),
        )
        together(
            scoring,
            weighing,
            sum_up(scores[ahead % len(scores)], tops[ahead % len(scores)], scale, results[-1]) if ahead is not None else iter(()),
        )
        for j, (top,) in zip(keys, found):
            tops[j % len(scores)] = top
        return results

    def stat_of(rows):
        stat = jnp.zeros((8, 128), jnp.float32)
        for j, (_, high, total) in enumerate(rows):
            for lane, value in enumerate((high[:8], high[8:], total[:8], total[8:])):
                stat = jnp.where(lanes == 4 * j + lane, value, stat)
        return stat

    def refill(copy, s):
        @pl.when(s < sequences)
        def _():
            copy(s).start()

    q_copy.wait()
    for s in range(EARLY, SLOTS):
        value_copy(s - EARLY).start()
        key_copy(s).start()
    for s in range(SLOTS - EARLY, SLOTS):
        value_copy(s).start()
    for j in range(LEAD):
        attend(0, [j], [])
        key_copy(SLOTS + j).start()

    def chunk(c, block):
        first = c * CHUNK
        rows = []
        for j in range(0, CHUNK, block):
            rows += attend(first, range(j + LEAD, j + LEAD + block), range(j, j + block))
            for i in range(j, j + block):
                refill(key_copy, first + i + LEAD + SLOTS)
                refill(value_copy, first + i + SLOTS)
        put(0, c, first, CHUNK, [row[0] for row in rows], stat_of(rows))

    @pl.loop(0, chunks)
    def _(c):
        first = c * CHUNK
        chunk(c, BLOCK)

        @pl.when(c == 0)
        def _():
            pl.semaphore_wait(barrier, len(others))

        send(0, c, first, CHUNK)

        @pl.when(c >= 1)
        def _():
            combine(0, c - 1, first - CHUNK, CHUNK)
            send(1, c - 1, first - CHUNK, CHUNK)

        @pl.when(c >= LAG)
        def _():
            combine(1, c - LAG, first - LAG * CHUNK, CHUNK)

    def end_whole(piece):
        a, z = END[piece] if piece < len(END) else (0, 0)
        return end_parts.at[pl.ds(0, len(others)), pl.ds(a, z - a)] if z else end_stats.at[pl.ds(0, len(others))]

    def end_send(piece):
        a, z = END[piece] if piece < len(END) else (0, 0)
        broadcast(end_parts.at[me, pl.ds(a, z - a)] if z else end_stats.at[me], end_sem.at[piece, 0], end_sem.at[piece, 1])

    def end_wait(piece, side):
        whole = end_whole(piece)
        pltpu.make_async_copy(whole, whole, end_sem.at[piece, side]).wait()

    first = sequences - TAIL
    rows = []
    for j in range(TAIL):
        rows[j:] = attend(first, [j + LEAD] if j + LEAD < TAIL else [], [j], j + 1 if j + 2 == TAIL else None)
        if j + LEAD + SLOTS < TAIL:
            key_copy(first + j + LEAD + SLOTS).start()
        if j + SLOTS < TAIL:
            value_copy(first + j + SLOTS).start()
        end_parts[me, j] = rows[j][0].astype(end_parts.dtype)
        if j + 2 == TAIL:
            end_stats[me] = stat_of(rows)
        if j + 1 == AFTER:
            combine(0, chunks - 1, first - CHUNK, CHUNK)
            send(1, chunks - 1, first - CHUNK, CHUNK)
        for piece, (_, z) in enumerate(END):
            if z == j + 1:
                end_send(piece)
        if j + 2 == TAIL:
            end_send(len(END))
    for c in range(chunks - LAG, chunks):
        combine(1, c, c * CHUNK, CHUNK)
    end_wait(len(END), 1)
    weight, _ = weights_of([end_stats[p] for p in range(side * side)], True)
    for piece, (a, z) in enumerate(END):
        end_wait(piece, 1)
        for j in range(a, z):
            out_ref[first + j] = sum_of(weight, lambda p: end_parts[p, j], j).astype(out_ref.dtype)

    for piece in range(len(END) + 1):
        end_wait(piece, 0)
    for ref, sem in ((parts.at[:, pl.ds(0, side - 1)], send_sem), (stats.at[:, :, pl.ds(0, side - 1)], stat_send_sem)):
        pltpu.make_async_copy(ref, ref, sem).wait()


def solution(mesh):
    side = math.isqrt(mesh.shape["sp"])

    def step(q, k, v):
        b, t, h, d = k.shape
        pieces = (b - TAIL) // CHUNK
        dma = pltpu.SemaphoreType.DMA
        return pl.pallas_call(
            functools.partial(kernel, side, d**-0.5),
            out_shape=pltpu.VMEM(q.shape, q.dtype),
            in_specs=[pl.BlockSpec(memory_space=pl.ANY)] * 3,
            out_specs=pl.BlockSpec(memory_space=pltpu.VMEM),
            scratch_shapes=[
                pltpu.VMEM((b, h, d), q.dtype),
                pltpu.VMEM((SLOTS, t * h, d), k.dtype),
                pltpu.VMEM((SLOTS, t * h, d), v.dtype),
                [pltpu.VMEM((2 * h, t * h // 2), jnp.float32)] * (2 * LEAD),
                pltpu.VMEM((2 * LEAD, 2 * h, TILE), jnp.float32),
                pltpu.VMEM((2, side, b - TAIL, h, d), jnp.bfloat16),
                pltpu.VMEM((2, pieces, side, 8, 128), jnp.float32),
                pltpu.VMEM((side * side, TAIL, h, d), jnp.bfloat16),
                pltpu.VMEM((side * side, 8, 128), jnp.float32),
                dma,
                dma((SLOTS,)),
                dma((SLOTS,)),
                dma,
                dma((2, pieces)),
                dma,
                dma((2, pieces)),
                dma((len(END) + 1, 2)),
            ],
            compiler_params=pltpu.CompilerParams(collective_id=0, has_side_effects=True, vmem_limit_bytes=60 * 2**20),
        )(q, k.reshape(b, t * h, d), v.reshape(b, t * h, d))

    return jax.shard_map(
        step,
        mesh=mesh,
        in_specs=(P("dp", None, None), P("dp", "sp", None, None), P("dp", "sp", None, None)),
        out_specs=P("dp", None, None),
        check_vma=False,
    )
```
